256 devices in a mesh: row: 32 (over x, y, z_lo), col: 8 (over z_hi, core).
Axes of the slice: x: 4, y: 4, z: 8 (z_hi: 4, z_lo: 2; z = z_hi * 2 + z_lo), core: 2. Of those that a mesh axis runs over, the one named last changes fastest.
Arguments:
- incident: bfloat16 [2, 65536, 512], P(None, ('row', 'col')), may hold values from -6 to 6
- near_tiles: bfloat16 [256, 2, 3, 2, 256, 256], P(('row', 'col')), may hold values from -0.15625 to 0.15625
- near_offsets: int32 [256, 3], P(('row', 'col')), may hold values from -2 to 2, as said below
- far_row: int32 [32, 8, 64], P('row', 'col'), may hold values from 0 to 7, as said below
- far_col: int32 [32, 8, 64], P('row', 'col'), may hold values from 0 to 31
- far_rank: int32 [32, 8, 64], P('row', 'col'), may hold values from 8 to 32, as said below
- far_count: int32 [32, 8], P('row', 'col'), may hold values from 8 to 64, as said below
- far_u: bfloat16 [32, 8, 2, 64, 2, 32, 256], P('row', 'col'), may hold values from -0.125 to 0.125
- far_v: bfloat16 [32, 8, 2, 64, 2, 32, 256], P('row', 'col'), may hold values from -0.25 to 0.25
Outputs:
- response: bfloat16 [2, 65536, 512], P(None, ('row', 'col'))
The draws below stay inside these ranges and needn't reach their ends.
Inputs may be any that keep to these rules, and one draw needn't show every extreme that they name: `near_offsets`: slot 0 of every tile is 0; the other slots of a tile hold distinct values among -2, -1, 1, 2. On one device the pairs (far_row, far_col) of all 64 slots are distinct, and every block (i, j) they name has circular tile distance 3 or more between i and j. `far_rank`: slot 0 of every device has rank 32. `far_count`: some device has all 64 slots live.
All inputs are finite; a program needn't handle non-finite values.
Results may differ from the reference program's by a relative error of at most 0.0035.
Values may be sent and summed in bfloat16 or wider, within the bound.
A program may use at most 192 MiB of HBM per device.

```python
import jax
import jax.numpy as jnp
from jax import lax

TILE = 256
RANK = 32
NEAR_SLOTS = 3
WAVES = 2
SOURCES = 256
FAR_SLOTS = 64
TILES = 256
PANELS = 65536
N_ROW = 32
N_COL = 8


def draw_near_offsets(key, part):
    tile_count = N_ROW * N_COL
    scores = jax.random.randint(jax.random.fold_in(key, 11), (tile_count, 4), 0, 1 << 20) * 4 + jnp.arange(4, dtype=jnp.int32)[None, :]
    ranking = jnp.argsort(scores, axis=1)
    offset_table = jnp.array([-2, -1, 1, 2], dtype=jnp.int32)
    picked = offset_table[ranking[:, :NEAR_SLOTS - 1]]
    return jnp.concatenate([jnp.zeros((tile_count, 1), jnp.int32), picked], axis=1).astype(jnp.int32)


def far_layout(key):
    pair_count = N_COL * N_ROW
    tile_count = N_ROW * N_COL
    pair_ids = jnp.arange(pair_count, dtype=jnp.int32)
    local_row = pair_ids // N_ROW
    col_device = pair_ids % N_ROW
    row_index = jnp.arange(N_ROW, dtype=jnp.int32)[:, None, None]
    col_index = jnp.arange(N_COL, dtype=jnp.int32)[None, :, None]
    row_tile = row_index * N_COL + local_row[None, None, :]
    col_tile = col_device[None, None, :] * N_COL + col_index
    forward_gap = (row_tile - col_tile) % tile_count
    circular = jnp.minimum(forward_gap, tile_count - forward_gap)
    random_part = jax.random.randint(jax.random.fold_in(key, 21), (N_ROW, N_COL, pair_count), 0, 1 << 19)
    scores = random_part * 1024 + pair_ids[None, None, :] + jnp.where(circular < 3, 1 << 30, 0)
    ranking = jnp.argsort(scores, axis=2)[:, :, :FAR_SLOTS]
    return ((ranking // N_ROW).astype(jnp.int32), (ranking % N_ROW).astype(jnp.int32))


def draw_far_row(key, part):
    return far_layout(key)[0]


def draw_far_col(key, part):
    return far_layout(key)[1]


def draw_far_rank(key, part):
    sampled = jax.random.randint(jax.random.fold_in(key, 31), (N_ROW, N_COL, FAR_SLOTS), max(1, RANK // 4), RANK + 1)
    leading = (jnp.arange(FAR_SLOTS, dtype=jnp.int32) == 0)[None, None, :]
    return jnp.where(leading, RANK, sampled).astype(jnp.int32)


def draw_far_count(key, part):
    lowest = max(1, FAR_SLOTS // 8)
    spread = FAR_SLOTS - lowest
    uniform_part = jax.random.randint(jax.random.fold_in(key, 41), (N_ROW, N_COL), 0, spread + 1)
    counts = lowest + uniform_part * uniform_part // spread
    fullest = jax.random.randint(jax.random.fold_in(key, 42), (), 0, N_ROW * N_COL)
    flat_index = jnp.arange(N_ROW * N_COL, dtype=jnp.int32).reshape(N_ROW, N_COL)
    return jnp.where(flat_index == fullest, FAR_SLOTS, counts).astype(jnp.int32)


def levels(rng, extent, pieces, least, high):
    def one(position, parts):
        draws = jax.random.uniform(jax.random.fold_in(jax.random.fold_in(rng, 6), position), (parts,), jnp.float32, least / len(pieces), high / len(pieces))
        return jnp.repeat(jnp.exp(draws), extent[position] // parts).reshape((-1,) + (1,) * (len(extent) - position - 1))

    loudness = one(*pieces[0])
    for cut in pieces[1:]:
        loudness = loudness * one(*cut)
    return loudness


def normal_values(own_key, extent, width, most, pieces=(), held_as=jnp.bfloat16):
    level = levels(own_key, extent, pieces, -0.22, 0.18) if pieces else 1.0
    drawn = jax.random.normal(own_key, extent, jnp.float32) * width * level
    return jnp.minimum(jnp.maximum(drawn, -most), most).astype(held_as)


def setup_inputs(seed: int = 0) -> dict:
    keys = jax.random.split(jax.random.key(seed), 10)
    return {
        "incident": normal_values(keys[0], (WAVES, PANELS, 2 * SOURCES), 1.0, 6.0, ((1, 256),)),
        "near_tiles": normal_values(keys[1], (TILES, WAVES, NEAR_SLOTS, 2, TILE, TILE), (2 * TILE * NEAR_SLOTS) ** -0.5, 0.15625, ((0, 256),)),
        "near_offsets": draw_near_offsets(jax.random.fold_in(keys[9], 71), 0),
        "far_row": draw_far_row(jax.random.fold_in(keys[9], 71), 0),
        "far_col": draw_far_col(jax.random.fold_in(keys[9], 71), 0),
        "far_rank": draw_far_rank(jax.random.fold_in(keys[9], 71), 0),
        "far_count": draw_far_count(jax.random.fold_in(keys[9], 71), 0),
        "far_u": normal_values(keys[7], (N_ROW, N_COL, WAVES, FAR_SLOTS, 2, RANK, TILE), (RANK * FAR_SLOTS) ** -0.5, 0.125, ((0, 32), (1, 8))),
        "far_v": normal_values(keys[8], (N_ROW, N_COL, WAVES, FAR_SLOTS, 2, RANK, TILE), (2 * TILE) ** -0.5, 0.25, ((0, 32), (1, 8))),
    }


def combine_parts(real_prod, imag_prod):
    half_width = real_prod.shape[-1] // 2
    return jnp.concatenate([real_prod[..., :half_width] - imag_prod[..., half_width:], real_prod[..., half_width:] + imag_prod[..., :half_width]], axis=-1)


def reference(incident, near_tiles, near_offsets, far_row, far_col, far_rank, far_count, far_u, far_v):
    tile_count = N_ROW * N_COL
    columns = incident.shape[-1]
    tiles_input = incident.reshape(WAVES, tile_count, TILE, columns)
    near_groups = near_tiles.reshape(N_ROW, N_COL, WAVES, NEAR_SLOTS, 2, TILE, TILE)
    offset_groups = near_offsets.reshape(N_ROW, N_COL, NEAR_SLOTS)
    slot_ids = jnp.arange(FAR_SLOTS, dtype=jnp.int32)
    rank_ids = jnp.arange(RANK, dtype=jnp.int32)
    block_ids = jnp.arange(N_COL, dtype=jnp.int32)

    def one_group(packed):
        group_index, near_part, offset_part, rows_part, cols_part, rank_part, count_part, u_part, v_part = packed
        own_tiles = group_index * N_COL + block_ids
        near_index = ((own_tiles[:, None] + offset_part) % tile_count).astype(jnp.int32)
        near_inputs = tiles_input[:, near_index].astype(jnp.float32)
        near_float = near_part.astype(jnp.float32)
        real_prod = jnp.einsum("awnpq,wanqc->wapc", near_float[:, :, :, 0], near_inputs)
        imag_prod = jnp.einsum("awnpq,wanqc->wapc", near_float[:, :, :, 1], near_inputs)
        result_rows = combine_parts(real_prod, imag_prod)
        for col_group in range(N_COL):
            col_tiles = (cols_part[col_group] * N_COL + col_group).astype(jnp.int32)
            live_mask = ((slot_ids < count_part[col_group])[:, None] & (rank_ids[None, :] < rank_part[col_group][:, None])).astype(jnp.float32)
            select = (rows_part[col_group][:, None] == block_ids[None, :]).astype(jnp.float32)
            for wave_index in range(WAVES):
                slot_tiles = tiles_input[wave_index, col_tiles].astype(jnp.float32)
                v_factor = v_part[col_group, wave_index].astype(jnp.float32)
                coefficients = combine_parts(jnp.einsum("fkq,fqc->fkc", v_factor[:, 0], slot_tiles), jnp.einsum("fkq,fqc->fkc", v_factor[:, 1], slot_tiles))
                coefficients = lax.optimization_barrier((coefficients * live_mask[:, :, None]).astype(jnp.bfloat16)).astype(jnp.float32)
                u_factor = u_part[col_group, wave_index].astype(jnp.float32)
                contrib = combine_parts(jnp.einsum("fkp,fkc->fpc", u_factor[:, 0], coefficients), jnp.einsum("fkp,fkc->fpc", u_factor[:, 1], coefficients))
                added = jnp.einsum("fa,fpc->apc", select, contrib, precision=lax.Precision.HIGHEST)
                result_rows = result_rows.at[wave_index].add(added)
        return result_rows.astype(jnp.bfloat16)

    grouped = lax.map(one_group, (jnp.arange(N_ROW, dtype=jnp.int32), near_groups, offset_groups, far_row, far_col, far_rank, far_count, far_u, far_v))
    return jnp.transpose(grouped, (1, 0, 2, 3, 4)).reshape(WAVES, tile_count * TILE, columns)
```

```python
import functools

import jax
import jax.numpy as jnp
from jax import lax
from jax.experimental import pallas as pl
from jax.experimental.pallas import tpu as pltpu
from jax.sharding import PartitionSpec as P

MESH = pl.DeviceIdType.MESH
BF16 = jnp.bfloat16
F32 = jnp.float32

TILE, RANK, SLOTS, WAVES, HALF = 256, 32, 64, 2, 256
WIDTH = 2 * HALF
N_ROW, N_COL, NEAR = 32, 8, 3
PACK = 4
GROUPS = (SLOTS + N_COL * (PACK - 1)) // PACK
HOPS = 8
ROWS = ((0, 128), (0, 128), (128, 128), (128, 128))
LAST = ((0, 64), (64, 64), (128, 64), (192, 64))

T_COL, T_RANK = 0, SLOTS
T_USLOT = T_RANK + SLOTS
T_CSLOT = T_USLOT + PACK * GROUPS
T_SAME = T_CSLOT + PACK * GROUPS
T_LAST = T_SAME + GROUPS
T_NEAR = T_LAST + N_COL
T_SIZE = T_NEAR + NEAR


def scalar_table(far_row, far_col, far_rank, far_count, near_offsets):
    i32 = jnp.int32
    slot = jnp.arange(SLOTS, dtype=i32)
    block = jnp.arange(N_COL, dtype=i32)
    earlier = (slot[:, None] > slot[None, :]) & (far_row[:, None] == far_row[None, :])
    place = jnp.sum(earlier.astype(i32), axis=1)
    count = jnp.sum((far_row[:, None] == block[None, :]).astype(i32), axis=0)
    groups = (count + PACK - 1) // PACK
    below = jnp.where(far_row[:, None] > block[None, :], groups[None, :], 0)
    dest = PACK * jnp.sum(below, axis=1) + place
    end = jnp.sum(jnp.where(block[:, None] >= block[None, :], groups[None, :], 0), axis=1)
    spot = jnp.arange(PACK * GROUPS, dtype=i32)
    hit = dest[None, :] == spot[:, None]
    uslot = jnp.sum(jnp.where(hit, slot[None, :], 0), axis=1)
    cslot = SLOTS + jnp.sum(jnp.where(hit, slot[None, :] - SLOTS, 0), axis=1)
    group = jnp.arange(GROUPS, dtype=i32)
    opens = ((end - groups)[None, :] == group[:, None]) & (groups[None, :] > 0)
    same = 1 - jnp.sum(opens.astype(i32), axis=1)
    last = jnp.where(groups > 0, end, 0)
    rank = jnp.where(slot < far_count, far_rank, 0)
    return jnp.concatenate([far_col, rank, uslot, cslot, same, last, near_offsets + 2]).astype(i32)


def mod(value, size):
    return lax.rem(value + size, size)


def body(
    table, x_hbm, near_hbm, u_hbm, v_hbm, out_ref,
    tiles0, tiles1, coef, ugrp, u_buf, v_buf, near_buf, near_x, near_acc, part,
    half_out, half_in, far_out, far_in,
    load_sem, ring_send, ring_recv, pair_send, pair_recv, near_send, near_recv,
    half_send, half_recv, far_send, far_recv,
):
    tiles = (tiles0, tiles1)
    r, c = lax.axis_index("row"), lax.axis_index("col")
    zl, xy = lax.rem(r, 2), r // 2
    y, x = lax.rem(xy, 4), xy // 4
    core, zh = lax.rem(c, 2), c // 2
    spot = (4 * x + lax.rem(x + y, 4), 4 * y + lax.rem(x + y, 4))

    def chip_at(ring, position):
        p = mod(position, 16)
        lead = p // 4
        trail = mod(lax.rem(p, 4) - lead, 4)
        return 4 * lead + trail if ring == 0 else 4 * trail + lead

    streams = ((0, 1), (0, -1), (1, 1), (1, -1))
    ring_next = [(chip_at(ring, spot[ring] + way) * 2 + zl, c) for ring, way in streams]
    pair = (r + 1 - 2 * zl, c)
    twin = (r, c + 1 - 2 * core)
    flat = r * N_COL + c
    shifts = (-2, -1, 1, 2)

    def flat_id(value):
        value = mod(value, N_ROW * N_COL)
        return (value // N_COL, lax.rem(value, N_COL))

    near_to = [flat_id(flat + shift) for shift in shifts]
    far_to = [(r, mod(zh + step, 4) * 2 + core) for step in (1, 2, 3)]

    loads = []
    for w in range(WAVES):
        loads.append(pltpu.make_async_copy(x_hbm.at[w], tiles[w].at[r], load_sem.at[w]))
    loads.append(pltpu.make_async_copy(x_hbm, near_x.at[2], load_sem.at[2]))
    loads.append(pltpu.make_async_copy(near_hbm, near_buf, load_sem.at[3]))
    loads.append(pltpu.make_async_copy(u_hbm, u_buf, load_sem.at[4]))
    loads.append(pltpu.make_async_copy(v_hbm, v_buf, load_sem.at[5]))
    for load in loads:
        load.start()

    barrier = pltpu.get_barrier_semaphore()
    peers = ring_next + [pair, twin] + near_to + far_to
    for peer in peers:
        pl.semaphore_signal(barrier, inc=1, device_id=peer, device_id_type=MESH)
    pl.semaphore_wait(barrier, len(peers))

    def remote(src, dst, send, recv, to):
        return pltpu.make_async_remote_copy(
            src_ref=src, dst_ref=dst, send_sem=send, recv_sem=recv, device_id=to, device_id_type=MESH
        )

    def pair_copy(w, tile):
        return remote(tiles[w].at[tile], tiles[w].at[tile], pair_send.at[w], pair_recv.at[w], pair)

    def ring_copy(w, k, sub, s, tile, rows):
        piece = tiles[w].at[tile, pl.ds(*rows[s])]
        return remote(piece, piece, ring_send.at[w, k, sub, s], ring_recv.at[w, k, sub, s], ring_next[s])

    def origin(s, k, sub):
        ring, way = streams[s]
        plane = zl if sub == 0 else 1 - zl
        return chip_at(ring, spot[ring] - way * k) * 2 + plane

    def ring_start(w, sub):
        for s in range(4):
            ring_copy(w, 0, sub, s, origin(s, 0, sub), ROWS).start()

    def ring_forward(w, k, sub, rows):
        for s in range(4):
            tile = origin(s, k, sub)
            ring_copy(w, k - 1, sub, s, tile, ROWS).wait_recv()
            ring_copy(w, k, sub, s, tile, rows).start()

    def near_copy(i):
        return remote(x_hbm, near_x.at[(4, 3, 1, 0)[i]], near_send.at[i], near_recv.at[i], near_to[i])

    def group_u(w, g):
        stack = [u_buf[w, table[T_USLOT + PACK * g + i]] for i in range(PACK)]
        ugrp[w, g] = jnp.concatenate(stack, axis=0).T

    def near_product(w):
        def rows(b, carry):
            here = pl.ds(pl.multiple_of(b * 64, 64), 64)
            real = jnp.zeros((64, WIDTH), F32)
            imag = jnp.zeros((64, WIDTH), F32)
            for n in range(NEAR):
                at = near_x[table[T_NEAR + n], w]
                real += jnp.dot(near_buf[w, n, 0, here], at, preferred_element_type=F32)
                imag += jnp.dot(near_buf[w, n, 1, here], at, preferred_element_type=F32)
            near_acc[w, here, :HALF] = real[:, :HALF] - imag[:, HALF:]
            near_acc[w, here, HALF:] = real[:, HALF:] + imag[:, :HALF]
            return carry

        lax.fori_loop(0, TILE // 64, rows, 0)

    rank_row = lax.broadcasted_iota(jnp.int32, (RANK, HALF), 0)

    def coefficients(w, s):
        at = tiles[w][table[T_COL + s]]
        prod = jnp.dot(v_buf[w, s], at, preferred_element_type=F32)
        live = rank_row < table[T_RANK + s]
        real = jnp.where(live, prod[:RANK, :HALF] - prod[RANK:, HALF:], 0.0).astype(BF16)
        imag = jnp.where(live, prod[:RANK, HALF:] + prod[RANK:, :HALF], 0.0).astype(BF16)
        coef[s, :RANK, :HALF] = real
        coef[s, :RANK, HALF:] = imag
        coef[s, RANK:, :HALF] = -imag
        coef[s, RANK:, HALF:] = real

    def row_sums(w, g):
        same = table[T_SAME + g].astype(F32)
        stack = [coef[table[T_CSLOT + PACK * g + i]] for i in range(PACK)]
        right = jnp.concatenate(stack, axis=0)
        for b in range(2):
            here = pl.ds(b * 128, 128)
            prod = jnp.dot(ugrp[w, g, here], right, preferred_element_type=F32)
            part[g + 1, here] = prod + same * part[g, here]

    def half_copy(w):
        return remote(half_out.at[w], half_in.at[w], half_send.at[w], half_recv.at[w], twin)

    def far_copy(w, d):
        return remote(far_out.at[w, d], far_in.at[w, d], far_send.at[w, d], far_recv.at[w, d], far_to[d])

    def reduce_pack(w):
        for i in range(4):
            a = 2 * i + 1 - core
            half_out[w, i] = part[table[T_LAST + a]].astype(BF16)

    def reduce_send(w):
        half_copy(w).wait_recv()
        for d in range(3):
            to = mod(zh + d + 1, 4)
            both = part[table[T_LAST + 2 * to + core]] + half_in[w, to].astype(F32)
            far_out[w, d] = both.astype(BF16)
        near_acc[w] += part[table[T_LAST + 2 * zh + core]] + half_in[w, zh].astype(F32)

    def reduce_start(w):
        for d in (1, 0, 2):
            far_copy(w, d).start()

    def finish(w):
        total = near_acc[w]
        for d in range(3):
            far_copy(w, d).wait_recv()
            total += far_in[w, d].astype(F32)
        out_ref[w] = total.astype(BF16)

    def many(first, last, step, *head):
        def one(i, carry):
            step(*head, i)
            return carry

        lax.fori_loop(first, last, one, 0)

    work = {(w, k, sub): [] for w in range(WAVES) for k in range(HOPS) for sub in range(2)}

    def at(w, k, sub, fn, *args):
        work[w, k, sub].append(functools.partial(fn, *args))

    def clear():
        coef[SLOTS] = jnp.zeros((2 * RANK, WIDTH), BF16)
        part[0] = jnp.zeros((TILE, WIDTH), F32)

    at(0, 0, 1, clear)
    at(0, 1, 0, lambda: loads[4].wait())
    for step in range(11):
        at(0, 1 + step // 2, step % 2, many, 4 * step, 4 * step + 4, lambda j: group_u(j // GROUPS, lax.rem(j, GROUPS)))
    at(0, 6, 1, lambda: [load.wait() for load in (loads[2], loads[3], loads[5])])
    at(0, 6, 1, lambda: [near_copy(i).wait_recv() for i in range(4)])
    at(0, 6, 1, near_product, 0)
    at(0, 7, 0, near_product, 1)
    for step in range(8):
        at(1, step // 2, step % 2, many, 8 * step, 8 * step + 8, coefficients, 0)
    for step in range(4):
        low, high = GROUPS * step // 4, GROUPS * (step + 1) // 4
        at(1, 4 + step // 2, step % 2, many, low, high, row_sums, 0)
    at(1, 5, 1, reduce_pack, 0)
    at(1, 6, 0, lambda: half_copy(0).start())
    at(1, 6, 1, reduce_send, 0)
    at(1, 7, 0, lambda: reduce_start(0))

    loads[0].wait()
    pair_copy(0, r).start()
    ring_start(0, 0)
    loads[1].wait()
    pair_copy(1, r).start()
    for i in range(4):
        near_copy(i).start()

    def pump(w):
        for k in range(HOPS):
            for sub in range(2):
                if k == 0 and sub == 0:
                    pass
                elif k == 0:
                    pair_copy(w, r + 1 - 2 * zl).wait_recv()
                    ring_start(w, 1)
                else:
                    ring_forward(w, k, sub, LAST if k == HOPS - 1 else ROWS)
                for item in work[w, k, sub]:
                    item()

    def drain(w):
        for sub in range(2):
            for s in range(4):
                ring_copy(w, HOPS - 1, sub, s, origin(s, HOPS, sub), LAST).wait_recv()

    pump(0)
    ring_start(1, 0)
    drain(0)
    pump(1)
    drain(1)

    many(0, SLOTS, coefficients, 1)
    many(0, GROUPS, row_sums, 1)
    reduce_pack(1)
    half_copy(1).start()
    finish(0)
    reduce_send(1)
    reduce_start(1)
    finish(1)

    for w in range(WAVES):
        pair_copy(w, r).wait_send()
        half_copy(w).wait_send()
        for d in range(3):
            far_copy(w, d).wait_send()
        for k in range(HOPS):
            for sub in range(2):
                for s in range(4):
                    ring_copy(w, k, sub, s, r, LAST if k == HOPS - 1 else ROWS).wait_send()
    for i in range(4):
        near_copy(i).wait_send()


def shards(incident, near_tiles, near_offsets, far_row, far_col, far_rank, far_count, far_u, far_v):
    table = scalar_table(far_row[0, 0], far_col[0, 0], far_rank[0, 0], far_count[0, 0], near_offsets[0])
    anywhere = pl.BlockSpec(memory_space=pl.ANY)
    dma = pltpu.SemaphoreType.DMA
    return pl.pallas_call(
        body,
        out_shape=jax.ShapeDtypeStruct((WAVES, TILE, WIDTH), BF16),
        in_specs=[pl.BlockSpec(memory_space=pltpu.SMEM)] + [anywhere] * 4,
        out_specs=pl.BlockSpec(memory_space=pltpu.VMEM),
        scratch_shapes=[
            pltpu.VMEM((N_ROW, TILE, WIDTH), BF16),
            pltpu.VMEM((N_ROW, TILE, WIDTH), BF16),
            pltpu.VMEM((SLOTS + 1, 2 * RANK, WIDTH), BF16),
            pltpu.VMEM((WAVES, GROUPS, TILE, PACK * 2 * RANK), BF16),
            pltpu.VMEM((WAVES, SLOTS, 2 * RANK, TILE), BF16),
            pltpu.VMEM((WAVES, SLOTS, 2 * RANK, TILE), BF16),
            pltpu.VMEM((WAVES, NEAR, 2, TILE, TILE), BF16),
            pltpu.VMEM((5, WAVES, TILE, WIDTH), BF16),
            pltpu.VMEM((WAVES, TILE, WIDTH), F32),
            pltpu.VMEM((GROUPS + 1, TILE, WIDTH), F32),
            pltpu.VMEM((WAVES, 4, TILE, WIDTH), BF16),
            pltpu.VMEM((WAVES, 4, TILE, WIDTH), BF16),
            pltpu.VMEM((WAVES, 3, TILE, WIDTH), BF16),
            pltpu.VMEM((WAVES, 3, TILE, WIDTH), BF16),
            dma((6,)),
            dma((WAVES, HOPS, 2, 4)),
            dma((WAVES, HOPS, 2, 4)),
            dma((WAVES,)),
            dma((WAVES,)),
            dma((4,)),
            dma((4,)),
            dma((WAVES,)),
            dma((WAVES,)),
            dma((WAVES, 3)),
            dma((WAVES, 3)),
        ],
        compiler_params=pltpu.CompilerParams(
            collective_id=0, has_side_effects=True, vmem_limit_bytes=67_043_328
        ),
    )(
        table,
        incident,
        near_tiles[0],
        far_u[0, 0].reshape(WAVES, SLOTS, 2 * RANK, TILE),
        far_v[0, 0].reshape(WAVES, SLOTS, 2 * RANK, TILE),
    )


def solution(mesh):
    in_specs = (
        P(None, ("row", "col"), None),
        P(("row", "col"), None, None, None, None, None),
        P(("row", "col"), None),
        P("row", "col", None),
        P("row", "col", None),
        P("row", "col", None),
        P("row", "col"),
        P("row", "col", None, None, None, None, None),
        P("row", "col", None, None, None, None, None),
    )
    out_specs = P(None, ("row", "col"), None)
    return jax.shard_map(shards, mesh=mesh, in_specs=in_specs, out_specs=out_specs, check_vma=False)
```

```python
import functools

import jax
import jax.numpy as jnp
from jax import lax
from jax.experimental import pallas as pl
from jax.experimental.pallas import tpu as pltpu
from jax.sharding import PartitionSpec as P

MESH = pl.DeviceIdType.MESH
BF16 = jnp.bfloat16
F32 = jnp.float32

TILE, RANK, SLOTS, WAVES, HALF = 256, 32, 64, 2, 256
WIDTH = 2 * HALF
N_ROW, N_COL, NEAR = 32, 8, 3
PACK = 4
GROUPS = (SLOTS + N_COL * (PACK - 1)) // PACK
HOPS = 8
ROWS = ((0, 128), (0, 128), (128, 128), (128, 128))
LAST = ((0, 64), (64, 64), (128, 64), (192, 64))

CHUNKS = 2 * WAVES
LANES = 128
PART = 2 * LANES
EAGER = 0.9
STARTS = (0.0, 0.0, 0.0, 52.0)
WIRE, HOP = 1.4, 2.6


def gather_order():
    paired = {q: max(2.8 * (q + 1), STARTS[q] - 5.2) + HOP for q in range(CHUNKS)}
    ready = {(q, sub): max(STARTS[q], paired[q] * sub) for q in range(CHUNKS) for sub in range(2)}
    hop = dict.fromkeys(ready, 0)
    now = free = 0.0
    when = []
    while hop:
        soon = max(now, free - WIRE, min(ready[x] for x in hop))
        q, sub = pick = min((x for x in hop if ready[x] <= soon + 1e-9), key=lambda x: (x[0], ready[x], x))
        when.append((soon, (q, hop[pick], sub)))
        now = max(now, ready[pick]) + 0.1
        free = max(now, free) + (WIRE if hop[pick] < HOPS - 1 else WIRE / 2)
        ready[pick] = free + HOP
        hop[pick] += 1
        if hop[pick] == HOPS:
            del hop[pick]
            if not any(x[0] == q for x in hop):
                when.append((free + HOP, ("drain", q)))
    when.sort(key=lambda x: x[0])
    return [(step, nxt - time) for (time, step), (nxt, _) in zip(when, when[1:] + when[-1:])]


def mod(value, size):
    return lax.rem(value + size, size)


def body(
    row_hbm, col_hbm, rank_hbm, count_hbm, offset_hbm, x_hbm, near_hbm, u_hbm, v_hbm, out_ref,
    tiles0, tiles1, tiles2, tiles3, near_x0, near_x1, near_x2, near_x3,
    coef, ugrp, u_buf, v_buf, near_buf, near_acc, part,
    half_out, half_in, far_out, far_in, held,
    row_buf, plan_buf, plan, far_col, far_rank, far_count, near_offset,
    small_sem, plan_sem, x_sem, load_sem, ring_send, ring_recv, pair_send, pair_recv, near_send, near_recv,
    half_send, half_recv, far_send, far_recv,
):
    tiles = (tiles0, tiles1, tiles2, tiles3)
    near_x = (near_x0, near_x1, near_x2, near_x3)
    r, c = lax.axis_index("row"), lax.axis_index("col")
    zl, xy = lax.rem(r, 2), r // 2
    y, x = lax.rem(xy, 4), xy // 4
    core, zh = lax.rem(c, 2), c // 2
    spot = (4 * x + lax.rem(x + y, 4), 4 * y + lax.rem(x + y, 4))

    def chip_at(ring, position):
        p = mod(position, 16)
        lead = p // 4
        trail = mod(lax.rem(p, 4) - lead, 4)
        return 4 * lead + trail if ring == 0 else 4 * trail + lead

    streams = ((0, 1), (0, -1), (1, 1), (1, -1))
    ring_next = [(chip_at(ring, spot[ring] + way) * 2 + zl, c) for ring, way in streams]
    pair_row = r + 1 - 2 * zl
    pair = (pair_row, c)
    twin = (r, c + 1 - 2 * core)
    far_up, far_down = ((r, mod(zh + step, 4) * 2 + core) for step in (1, -1))

    line = 4 * zl + zh

    def on_line(place):
        place = mod(place, 8)
        return (2 * xy + place // 4, 2 * lax.rem(place, 4) + core)

    near_to = (on_line(line + 1), on_line(line - 1), twin, twin)
    up_wraps, down_wraps = line == 7, line == 0
    up_row = mod(r - 2 * (line // 7), N_ROW)
    down_row = mod(r + 2 * (1 - (line + 6) // 7), N_ROW)

    small = [
        pltpu.make_async_copy(src, dst, small_sem.at[i])
        for i, (src, dst) in enumerate((
            (row_hbm, row_buf), (col_hbm, far_col), (rank_hbm, far_rank), (count_hbm, far_count), (offset_hbm, near_offset),
        ))
    ]
    x_loads = []
    for q in range(CHUNKS):
        for i in range(2):
            src = x_hbm.at[q // 2, :, pl.ds(HALF * i + LANES * (q % 2), LANES)]
            for n, dst in enumerate((tiles[q].at[r], near_x[q].at[2])):
                x_loads.append(pltpu.make_async_copy(src, dst.at[:, pl.ds(LANES * i, LANES)], x_sem.at[q, n]))
    loads = [
        pltpu.make_async_copy(src, dst, load_sem.at[i])
        for i, (src, dst) in enumerate(((near_hbm, near_buf), (u_hbm, u_buf), (v_hbm, v_buf)))
    ]
    for load in x_loads + small + loads:
        load.start()

    barrier = pltpu.get_barrier_semaphore()
    peers = ring_next + [pair, twin] + list(near_to[:2]) + [far_up, far_down]
    for peer in peers:
        pl.semaphore_signal(barrier, inc=1, device_id=peer, device_id_type=MESH)
    pl.semaphore_wait(barrier, len(peers))

    def remote(src, dst, send, recv, to):
        return pltpu.make_async_remote_copy(
            src_ref=src, dst_ref=dst, send_sem=send, recv_sem=recv, device_id=to, device_id_type=MESH
        )

    def pair_copy(q, tile):
        return remote(tiles[q].at[tile], tiles[q].at[tile], pair_send.at[q], pair_recv.at[q], pair)

    def ring_copy(q, k, sub, s, tile, rows):
        piece = tiles[q].at[tile, pl.ds(*rows[s])]
        return remote(piece, piece, ring_send.at[q], ring_recv.at[q, k, sub], ring_next[s])

    def origin(s, k, sub):
        ring, way = streams[s]
        plane = zl if sub == 0 else 1 - zl
        return chip_at(ring, spot[ring] - way * k) * 2 + plane

    def ring_wait(q, k, sub):
        both = tiles[q].at[pl.ds(0, 1 if k == HOPS - 1 else 2)]
        remote(both, both, ring_send.at[q], ring_recv.at[q, k, sub], ring_next[0]).wait_recv()

    def forward(q, k, sub):
        rows = LAST if k == HOPS - 1 else ROWS
        if k > 0:
            ring_wait(q, k - 1, sub)
        elif sub == 1:
            pair_copy(q, pair_row).wait_recv()
        for s in range(4):
            ring_copy(q, k, sub, s, origin(s, k, sub), rows).start()

    def ring_sent(q):
        everything = tiles[q].at[pl.ds(0, 30)]
        remote(everything, everything, ring_send.at[q], ring_recv.at[q, 0, 0], ring_next[0]).wait_send()

    def drain(q):
        for sub in range(2):
            ring_wait(q, HOPS - 1, sub)

    def near_copy(q, i):
        src = (
            tiles[q].at[up_row], tiles[q].at[down_row], tiles[q].at[r], near_x[q].at[4 - 4 * core],
        )[i]
        dst = near_x[q].at[(0, 4, 1 + 2 * core, 3 - 2 * core)[i]]
        return remote(src, dst, near_send.at[q], near_recv.at[q, i], near_to[i])

    def near_early(q):
        near_copy(q, 2).start()

        @pl.when(jnp.logical_not(up_wraps))
        def _():
            near_copy(q, 0).start()

        @pl.when(jnp.logical_not(down_wraps))
        def _():
            near_copy(q, 1).start()

    def near_late(q):
        @pl.when(up_wraps)
        def _():
            near_copy(q, 0).start()

        @pl.when(down_wraps)
        def _():
            near_copy(q, 1).start()

    def near_relay(q):
        near_copy(q, 0).wait_recv()
        near_copy(q, 1).wait_recv()
        near_copy(q, 3).start()

    def near_arrived(q):
        near_copy(q, 2).wait_recv()
        near_copy(q, 3).wait_recv()

    def make_plan():
        small[0].wait()

        def number(shape, dim):
            return lax.broadcasted_iota(jnp.int32, shape, dim)

        def total(mask, value, axis):
            return jnp.sum(jnp.where(mask, value, 0), axis=axis, keepdims=True, dtype=jnp.int32)

        square, wide, low = (SLOTS, SLOTS), (SLOTS, 128), (N_COL, 128)
        rows_on_lanes = jnp.broadcast_to(row_buf[...], square)
        i, j = number(square, 0), number(square, 1)
        rows = total(i == j, rows_on_lanes, 1)
        place = total((rows_on_lanes == rows) & (j < i), 1, 1)
        a = number(wide, 1)
        count = total(a == rows, 1, 0)
        groups = lax.shift_right_logical(count + (PACK - 1), 2)
        dest = PACK * total(a < rows, jnp.broadcast_to(groups, wide), 1) + place
        slot = number(wide, 0)
        uslot = total(dest == a, slot, 0)
        cslot = SLOTS + total(dest == a, slot - SLOTS, 0)
        b, lane = number(low, 0), number(low, 1)
        groups_low = jnp.broadcast_to(groups, low)
        own = total(b == lane, groups_low, 1)
        end = total(lane <= b, groups_low, 1)
        same = 1 - total((end - own == lane) & (own > 0), 1, 0)
        last = total(b == lane, jnp.where(own > 0, end, 0), 0)
        plan_buf[...] = jnp.concatenate([uslot, cslot, same, last] * 2, axis=0)
        copy = pltpu.make_async_copy(plan_buf, plan, plan_sem)
        copy.start()
        coef[SLOTS] = jnp.zeros((2 * RANK, PART), BF16)
        part[0] = jnp.zeros((TILE, PART), F32)
        copy.wait()

    def within(index, most):
        return jnp.minimum(jnp.maximum(index, 0), most)

    def group_u(w, g):
        stack = [u_buf[w, within(plan[0, PACK * g + i], SLOTS - 1)] for i in range(PACK)]
        ugrp[w, g] = jnp.concatenate(stack, axis=0).T

    def near_product(q):
        w = q // 2

        def rows(b, carry):
            here = pl.ds(pl.multiple_of(b * 128, 128), 128)
            real = jnp.zeros((128, PART), F32)
            imag = jnp.zeros((128, PART), F32)
            for n in range(NEAR):
                at = near_x[q][near_offset[0, n] + 2]
                real += jnp.dot(near_buf[w, n, 0, here], at, preferred_element_type=F32)
                imag += jnp.dot(near_buf[w, n, 1, here], at, preferred_element_type=F32)
            near_acc[q, here, :LANES] = real[:, :LANES] - imag[:, LANES:]
            near_acc[q, here, LANES:] = real[:, LANES:] + imag[:, :LANES]
            return carry

        lax.fori_loop(0, TILE // 128, rows, 0)

    rank_row = lax.broadcasted_iota(jnp.int32, (RANK, LANES), 0)

    def coefficients(q, s):
        at = tiles[q][far_col[0, s]]
        prod = jnp.dot(v_buf[q // 2, s], at, preferred_element_type=F32)
        live = rank_row < jnp.where(s < far_count[0, 0], far_rank[0, s], 0)
        real = jnp.where(live, prod[:RANK, :LANES] - prod[RANK:, LANES:], 0.0).astype(BF16)
        imag = jnp.where(live, prod[:RANK, LANES:] + prod[RANK:, :LANES], 0.0).astype(BF16)
        coef[s, :RANK, :LANES] = real
        coef[s, :RANK, LANES:] = imag
        coef[s, RANK:, :LANES] = -imag
        coef[s, RANK:, LANES:] = real

    def row_sums(q, g):
        same = plan[2, g].astype(F32)
        stack = [coef[within(plan[1, PACK * g + i], SLOTS)] for i in range(PACK)]
        right = jnp.concatenate(stack, axis=0)
        prod = jnp.dot(ugrp[q // 2, g], right, preferred_element_type=F32)
        part[g + 1] = prod + same * part[g]

    def row_part(a):
        return part[within(plan[3, a], GROUPS)]

    def half_copy(q, i):
        return remote(half_out.at[q, i], half_in.at[q, i], half_send.at[q], half_recv.at[q, i], twin)

    upper, lower = pl.ds(0, 128), pl.ds(128, 128)
    moves = ((1, upper, far_up), (1, lower, far_down), (0, lower, far_up), (2, upper, far_down), (0, upper, far_up), (2, lower, far_down))

    def far_copy(q, m):
        d, rows, to = moves[m]
        return remote(far_out.at[q, d, rows], far_in.at[q, d, rows], far_send.at[q], far_recv.at[q, m], to)

    turns = [mod(zh + step, 4) for step in (2, 1, 3, 0)]

    def reduce_pack(q):
        for n, i in enumerate(turns):
            half_out[q, i] = row_part(2 * i + 1 - core).astype(BF16)
            if n:
                half_copy(q, turns[n - 1]).start()
        half_copy(q, turns[3]).start()

    def reduce_pass(q):
        for n, i in enumerate(turns):
            half_copy(q, i).wait_recv()
            both = row_part(2 * i + core) + half_in[q, i].astype(F32)
            if n == 0:
                far_out[q, 1] = both.astype(BF16)
            elif n == 1:
                far_out[q, 0, lower] = both[128:].astype(BF16)
                held[0] = both[:128]
                far_copy(q, 0).start()
                far_copy(q, 1).start()
            elif n == 2:
                far_out[q, 2, upper] = both[:128].astype(BF16)
                held[1] = both[128:]
                far_copy(q, 2).start()
            else:
                near_acc[q] += both
                far_copy(q, 3).start()

    def reduce_relay(q):
        far_copy(q, 0).wait_recv()
        far_out[q, 0, upper] = (held[0] + far_in[q, 1, upper].astype(F32)).astype(BF16)
        far_copy(q, 1).wait_recv()
        far_out[q, 2, lower] = (held[1] + far_in[q, 1, lower].astype(F32)).astype(BF16)
        far_copy(q, 4).start()
        far_copy(q, 5).start()

    def finish(q):
        for m in (2, 3, 4, 5):
            far_copy(q, m).wait_recv()
        total = near_acc[q] + far_in[q, 0].astype(F32) + far_in[q, 2].astype(F32)
        here = LANES * (q % 2)
        out_ref[q // 2, :, here : here + LANES] = total[:, :LANES].astype(BF16)
        out_ref[q // 2, :, HALF + here : HALF + here + LANES] = total[:, LANES:].astype(BF16)

    def many(first, last, step, *head, unroll=1):
        def one(i, carry):
            for n in range(unroll):
                step(*head, i * unroll + n)
            return carry

        lax.fori_loop(first // unroll, last // unroll, one, 0)

    def tag(name, cost, fn, *args, **kw):
        def run():
            with jax.named_scope(name):
                fn(*args, **kw)

        return cost, run

    def far_work(q):
        yield from (tag(f"V{q}", 0.42, many, 8 * i, 8 * i + 8, coefficients, q, unroll=4) for i in range(SLOTS // 8))
        if q:
            yield tag(f"rel{q - 1}", 0.3, reduce_relay, q - 1)
        yield tag(f"nrel{q}", 0.1, near_relay, q)
        yield tag(f"U{q}", 0.7, many, 0, 6, row_sums, q, unroll=2)
        yield tag(f"U{q}", 0.7, many, 6, 12, row_sums, q, unroll=2)
        yield tag(f"U{q}", 0.7, many, 12, 18, row_sums, q, unroll=2)
        yield tag(f"U{q}", 0.5, many, 18, GROUPS, row_sums, q, unroll=2)
        yield tag(f"pack{q}", 0.3, reduce_pack, q)
        yield tag(f"near{q}", 0.6, near_all, q)
        yield tag(f"pass{q}", 0.7, reduce_pass, q)

    def near_all(q):
        near_arrived(q)
        near_product(q)

    def pair_start(q):
        pair_copy(q, r).start()

    def near_own():
        for q in range(CHUNKS):
            pltpu.make_async_copy(near_x[q].at[2], near_x[q].at[2], x_sem.at[q, 1]).wait()

    def early():
        yield tag("plan", 1.2, make_plan)
        yield tag("lu", 0.1, lambda: loads[1].wait())
        for i in range(11):
            yield tag("ugrp", 0.4, many, 4 * i, 4 * i + 4, lambda n: group_u(n // GROUPS, lax.rem(n, GROUPS)))
        yield tag("ld", 0.1, lambda: [load.wait() for load in small[1:] + [loads[0], loads[2]]])
        yield tag("ldx", 0.1, near_own)

    def load_chunk(q):
        pltpu.make_async_copy(tiles[q].at[r], tiles[q].at[r], x_sem.at[q, 0]).wait()

    load_chunk(0)
    pair_copy(0, r).start()
    forward(0, 0, 0)
    load_chunk(1)
    pair_copy(1, r).start()
    forward(1, 0, 0)
    load_chunk(2)
    load_chunk(3)
    queue = list(early())
    later = [
        (9, near_early, 0), (13, pair_start, 2), (18, near_early, 1), (24, pair_start, 3), (28, near_early, 2), (36, near_early, 3),
    ]
    time = 0.0
    credit = 0.0
    for step, gap in gather_order():
        if step[0] == "drain":
            with jax.named_scope(f"drain{step[1]}"):
                drain(step[1])
            if step[1] < CHUNKS - 1:
                queue += far_work(step[1])
        elif step not in ((0, 0, 0), (1, 0, 0)):
            with jax.named_scope("F%d%d%d" % step):
                forward(*step)
            if step[1:] == (6, 1):
                near_late(step[0])
        time += gap
        while later and later[0][0] <= time:
            _, send, q = later.pop(0)
            send(q)
        credit = min(credit + EAGER * gap, 3.0)
        while queue and credit >= queue[0][0] * 0.6:
            credit -= queue[0][0]
            queue.pop(0)[1]()
    for _, run in queue + list(far_work(CHUNKS - 1)):
        run()
    with jax.named_scope("rel3"):
        reduce_relay(CHUNKS - 1)
    with jax.named_scope("sent"):
        for q in range(CHUNKS):
            ring_sent(q)
            pair_copy(q, r).wait_send()
            remote(half_out.at[q], half_in.at[q], half_send.at[q], half_recv.at[q, 0], twin).wait_send()
            four = near_x[q].at[pl.ds(0, 4)]
            remote(four, four, near_send.at[q], near_recv.at[q, 0], twin).wait_send()
    for q in range(CHUNKS):
        with jax.named_scope(f"fin{q}"):
            finish(q)
            remote(far_out.at[q], far_in.at[q], far_send.at[q], far_recv.at[q, 0], far_up).wait_send()


def shards(incident, near_tiles, near_offsets, far_row, far_col, far_rank, far_count, far_u, far_v):
    dma = pltpu.SemaphoreType.DMA
    return pl.pallas_call(
        body,
        out_shape=jax.ShapeDtypeStruct((WAVES, TILE, WIDTH), BF16),
        in_specs=[pl.BlockSpec(memory_space=pl.ANY)] * 9,
        out_specs=pl.BlockSpec(memory_space=pltpu.VMEM),
        scratch_shapes=[pltpu.VMEM((N_ROW, TILE, PART), BF16)] * CHUNKS
        + [pltpu.VMEM((5, TILE, PART), BF16)] * CHUNKS
        + [
            pltpu.VMEM((SLOTS + 1, 2 * RANK, PART), BF16),
            pltpu.VMEM((WAVES, GROUPS, TILE, PACK * 2 * RANK), BF16),
            pltpu.VMEM((WAVES, SLOTS, 2 * RANK, TILE), BF16),
            pltpu.VMEM((WAVES, SLOTS, 2 * RANK, TILE), BF16),
            pltpu.VMEM((WAVES, NEAR, 2, TILE, TILE), BF16),
            pltpu.VMEM((CHUNKS, TILE, PART), F32),
            pltpu.VMEM((GROUPS + 1, TILE, PART), F32),
            pltpu.VMEM((CHUNKS, 4, TILE, PART), BF16),
            pltpu.VMEM((CHUNKS, 4, TILE, PART), BF16),
            pltpu.VMEM((CHUNKS, 3, TILE, PART), BF16),
            pltpu.VMEM((CHUNKS, 3, TILE, PART), BF16),
            pltpu.VMEM((2, 128, PART), F32),
            pltpu.VMEM((1, SLOTS), jnp.int32),
            pltpu.VMEM((8, 128), jnp.int32),
            pltpu.SMEM((8, 128), jnp.int32),
            pltpu.SMEM((1, SLOTS), jnp.int32),
            pltpu.SMEM((1, SLOTS), jnp.int32),
            pltpu.SMEM((1, 1), jnp.int32),
            pltpu.SMEM((1, NEAR), jnp.int32),
            dma((5,)),
            dma,
            dma((CHUNKS, 2)),
            dma((3,)),
            dma((CHUNKS,)),
            dma((CHUNKS, HOPS, 2)),
            dma((CHUNKS,)),
            dma((CHUNKS,)),
            dma((CHUNKS,)),
            dma((CHUNKS, 4)),
            dma((CHUNKS,)),
            dma((CHUNKS, 4)),
            dma((CHUNKS,)),
            dma((CHUNKS, 6)),
        ],
        compiler_params=pltpu.CompilerParams(
            collective_id=0, has_side_effects=True, vmem_limit_bytes=67_043_328
        ),
    )(
        far_row[0],
        far_col[0],
        far_rank[0],
        far_count,
        near_offsets,
        incident,
        near_tiles[0],
        far_u[0, 0].reshape(WAVES, SLOTS, 2 * RANK, TILE),
        far_v[0, 0].reshape(WAVES, SLOTS, 2 * RANK, TILE),
    )


def solution(mesh):
    in_specs = (
        P(None, ("row", "col"), None),
        P(("row", "col"), None, None, None, None, None),
        P(("row", "col"), None),
        P("row", "col", None),
        P("row", "col", None),
        P("row", "col", None),
        P("row", "col"),
        P("row", "col", None, None, None, None, None),
        P("row", "col", None, None, None, None, None),
    )
    out_specs = P(None, ("row", "col"), None)
    return jax.shard_map(shards, mesh=mesh, in_specs=in_specs, out_specs=out_specs, check_vma=False)
```

```python
import functools

import jax
import jax.numpy as jnp
from jax import lax
from jax.experimental import pallas as pl
from jax.experimental.pallas import tpu as pltpu
from jax.sharding import PartitionSpec as P

MESH = pl.DeviceIdType.MESH
BF16 = jnp.bfloat16
F32 = jnp.float32

TILE, RANK, SLOTS, WAVES, HALF = 256, 32, 64, 2, 256
WIDTH = 2 * HALF
N_ROW, N_COL, NEAR = 32, 8, 3
PACK = 4
GROUPS = (SLOTS + N_COL * (PACK - 1)) // PACK
HOPS = 8
ROWS = ((0, 128), (0, 128), (128, 128), (128, 128))
LAST = ((0, 64), (64, 64), (128, 64), (192, 64))

CHUNKS = 2 * WAVES
LANES = 128
PART = 2 * LANES
STARTS = (0.0, 0.0, 0.0, 44.0)
WIRE, HOP = 1.4, 2.6


SHORT = {0: 6, 1: 6}
CROSS_TIME = 10.0
QUEUE = 1.5
TWIN_TIME, RELAY_TIME, FAR_TIME, NEAR_TIME = 1.7, 7.0, 7.0, 2.5
BUSY = 6.0
V_PIECES, U_PIECES, G_PIECES = 8, 2, 11
V_UNROLL, U_UNROLL = 8, 11
U_COST = 2.2


def hops_of(q, sub):
    return SHORT.get(q, HOPS) if sub == 1 else HOPS


def work_items():
    items = {("plan",): (0, 0.9, {}), ("u_loaded",): (1, 0.1, {("plan",): 2.0})}
    for i in range(G_PIECES):
        items["group", i] = (2, 0.39, {("u_loaded",): 0.0})
    items["loaded",] = (3, 0.1, {("group", G_PIECES - 1): 0.0})
    for time, name in ((9, ("near_early", 0)), (13, ("pair", 2)), (18, ("near_early", 1)), (24, ("pair", 3)), (28, ("near_early", 2)), (36, ("near_early", 3))):
        items[name] = (-1, 0.05, {("start",): time})
    for q in range(CHUNKS):
        for i in range(V_PIECES):
            items["V", q, i] = (10 * q + 10, 2.5 / V_PIECES, {("drain", q): 0.0, ("loaded",): 0.0, ("U", q - 1, U_PIECES - 1): 0.0})
        for i in range(U_PIECES):
            items["U", q, i] = (10 * q + 11, U_COST / U_PIECES, {("V", q, V_PIECES - 1): 0.0, ("pass", q - 2): 0.0})
        items["pack", q] = (10 * q + 12, 0.3, {("U", q, U_PIECES - 1): 0.0})
        items["pass", q] = (10 * q + 13, 0.6, {("pack", q): TWIN_TIME, ("relay", q - 2): 0.0})
        items["relay", q] = (10 * q + 14, 0.25, {("pass", q): RELAY_TIME + BUSY * (q < 2)})
        items["near_relay", q] = (10 * q + 15, 0.1, {("drain", q): 1.0})
        items["near", q] = (100 + q, 0.55, {("near_relay", q): NEAR_TIME, ("loaded",): 0.0})
        items["finish", q] = (110 + q, 0.3, {("relay", q): FAR_TIME, ("near", q): 0.0, ("drain", CHUNKS - 1): 0.0})
    return items


def schedule():
    paired = {q: max(2.8 * (q + 1), STARTS[q] - 5.2) + HOP for q in range(CHUNKS)}
    ready = {(q, sub): max(STARTS[q], paired[q] * sub) for q in range(CHUNKS) for sub in range(2)}
    hop = dict.fromkeys(ready, 0)
    here = {}
    items = work_items()
    ended = {("start",): 0.0}
    now = free = 0.0
    order = []
    while hop or items:
        ripe = [x for x in hop if ready[x] <= now + 1e-9]
        if ripe and free - now <= QUEUE:
            q, sub = pick = min(ripe, key=lambda x: (x[0], ready[x], x))
            order.append(("step", q, hop[pick], sub))
            now += 0.12
            free = max(now, free) + (WIRE if hop[pick] < HOPS - 1 else WIRE / 2)
            ready[pick] = free + HOP
            hop[pick] += 1
            if hop[pick] == hops_of(q, sub):
                del hop[pick]
                here[pick] = ready[pick]
                if sub == 0 and q in SHORT:
                    items["cross", q] = (-2, 0.1, {("start",): ready[pick]})
                    here[pick] += CROSS_TIME
                if (q, 0) in here and (q, 1) in here:
                    items["drain", q] = (-2, 0.05, {("start",): max(here[q, 0], here[q, 1])})
            continue
        open_at = {}
        for name, (rank, cost, after) in items.items():
            known = {k: v for k, v in after.items() if k[-1] != -1 and k[1:2] != (-1,) and k[1:2] != (-2,)}
            if all(k in ended for k in known):
                open_at[name] = max([0.0] + [ended[k] + v for k, v in known.items()])
        can = [x for x in open_at if open_at[x] <= now + 1e-9]
        if can:
            name = min(can, key=lambda x: (items[x][0], [n for n in x[1:]]))
            order.append(name)
            now += items.pop(name)[1]
            ended[name] = now
            continue
        soon = [open_at[x] for x in open_at] + [max(ready[x], free - QUEUE) for x in hop]
        now = max(now + 1e-6, min(soon))
    return order


def mod(value, size):
    return lax.rem(value + size, size)


def body(
    row_hbm, col_hbm, rank_hbm, count_hbm, offset_hbm, x_hbm, near_hbm, u_hbm, v_hbm, out_hbm,
    tiles0, tiles1, tiles2, tiles3, near_x0, near_x1, near_x2, near_x3,
    coef, ugrp, u_buf, v_buf, near_buf, near_acc, part,
    half_out, half_in, far_out, far_in, held, own_acc, out_buf,
    row_buf, plan_buf, plan, far_col, far_rank, far_count, near_offset,
    small_sem, plan_sem, x_sem, load_sem, ring_send, ring_recv, pair_send, pair_recv, near_send, near_recv,
    half_send, half_recv, far_send, far_recv, cross_send, cross_recv, out_sem,
):
    tiles = (tiles0, tiles1, tiles2, tiles3)
    near_x = (near_x0, near_x1, near_x2, near_x3)
    r, c = lax.axis_index("row"), lax.axis_index("col")
    zl, xy = lax.rem(r, 2), r // 2
    y, x = lax.rem(xy, 4), xy // 4
    core, zh = lax.rem(c, 2), c // 2
    spot = (4 * x + lax.rem(x + y, 4), 4 * y + lax.rem(x + y, 4))

    def chip_at(ring, position):
        p = mod(position, 16)
        lead = p // 4
        trail = mod(lax.rem(p, 4) - lead, 4)
        return 4 * lead + trail if ring == 0 else 4 * trail + lead

    streams = ((0, 1), (0, -1), (1, 1), (1, -1))
    ring_next = [(chip_at(ring, spot[ring] + way) * 2 + zl, c) for ring, way in streams]
    pair_row = r + 1 - 2 * zl
    pair = (pair_row, c)
    twin = (r, c + 1 - 2 * core)
    far_up, far_down = ((r, mod(zh + step, 4) * 2 + core) for step in (1, -1))

    line = 4 * zl + zh

    def on_line(place):
        place = mod(place, 8)
        return (2 * xy + place // 4, 2 * lax.rem(place, 4) + core)

    near_to = (on_line(line + 1), on_line(line - 1), twin, twin)
    up_wraps, down_wraps = line == 7, line == 0
    up_row = mod(r - 2 * (line // 7), N_ROW)
    down_row = mod(r + 2 * (1 - (line + 6) // 7), N_ROW)

    small = [
        pltpu.make_async_copy(src, dst, small_sem.at[i])
        for i, (src, dst) in enumerate((
            (row_hbm, row_buf), (col_hbm, far_col), (rank_hbm, far_rank), (count_hbm, far_count), (offset_hbm, near_offset),
        ))
    ]
    x_loads = []
    for q in range(CHUNKS):
        for i in range(2):
            src = x_hbm.at[q // 2, :, pl.ds(HALF * i + LANES * (q % 2), LANES)]
            for n, dst in enumerate((tiles[q].at[r], near_x[q].at[2])):
                x_loads.append(pltpu.make_async_copy(src, dst.at[:, pl.ds(LANES * i, LANES)], x_sem.at[q, n]))
    loads = [
        pltpu.make_async_copy(src, dst, load_sem.at[i])
        for i, (src, dst) in enumerate(((near_hbm, near_buf), (u_hbm, u_buf), (v_hbm, v_buf)))
    ]
    for load in x_loads + small + loads:
        load.start()

    barrier = pltpu.get_barrier_semaphore()
    peers = ring_next + [pair, twin] + list(near_to[:2]) + [far_up, far_down]
    for peer in peers:
        pl.semaphore_signal(barrier, inc=1, device_id=peer, device_id_type=MESH)
    pl.semaphore_wait(barrier, len(peers))

    def remote(src, dst, send, recv, to):
        return pltpu.make_async_remote_copy(
            src_ref=src, dst_ref=dst, send_sem=send, recv_sem=recv, device_id=to, device_id_type=MESH
        )

    def pair_copy(q, tile):
        return remote(tiles[q].at[tile], tiles[q].at[tile], pair_send.at[q], pair_recv.at[q], pair)

    def ring_copy(q, k, sub, s, tile, rows):
        piece = tiles[q].at[tile, pl.ds(*rows[s])]
        return remote(piece, piece, ring_send.at[q], ring_recv.at[q, k, sub], ring_next[s])

    def origin(s, k, sub):
        ring, way = streams[s]
        plane = zl if sub == 0 else 1 - zl
        return chip_at(ring, spot[ring] - way * k) * 2 + plane

    def ring_wait(q, k, sub):
        both = tiles[q].at[pl.ds(0, 1 if k == HOPS - 1 else 2)]
        remote(both, both, ring_send.at[q], ring_recv.at[q, k, sub], ring_next[0]).wait_recv()

    def forward(q, k, sub):
        rows = LAST if k == HOPS - 1 else ROWS
        if k > 0:
            ring_wait(q, k - 1, sub)
        elif sub == 1:
            pair_copy(q, pair_row).wait_recv()
        for s in range(4):
            ring_copy(q, k, sub, s, origin(s, k, sub), rows).start()

    def ring_sent(q):
        everything = tiles[q].at[pl.ds(0, 15 + 2 * SHORT[q] if q in SHORT else 30)]
        remote(everything, everything, ring_send.at[q], ring_recv.at[q, 0, 0], ring_next[0]).wait_send()

    def cross_start(q, k):
        for s in range(4 if k < HOPS else 1):
            piece = tiles[q].at[origin(s, k, 0)]
            piece = piece.at[pl.ds(*ROWS[s])] if k < HOPS else piece
            remote(piece, piece, cross_send.at[q], cross_recv.at[q, HOPS - k], pair).start()

    def cross_wait(q):
        for k in range(SHORT[q] + 1, HOPS + 1):
            got = tiles[q].at[pl.ds(0, 2 if k < HOPS else 1)]
            remote(got, got, cross_send.at[q], cross_recv.at[q, HOPS - k], pair).wait_recv()

    def cross(q):
        ring_wait(q, HOPS - 1, 0)
        cross_start(q, HOPS)

    def drain(q):
        if q in SHORT:
            ring_wait(q, SHORT[q] - 1, 1)
            cross_wait(q)
        else:
            ring_wait(q, HOPS - 1, 0)
            ring_wait(q, HOPS - 1, 1)

    def near_copy(q, i):
        src = (
            tiles[q].at[up_row], tiles[q].at[down_row], tiles[q].at[r], near_x[q].at[4 - 4 * core],
        )[i]
        dst = near_x[q].at[(0, 4, 1 + 2 * core, 3 - 2 * core)[i]]
        return remote(src, dst, near_send.at[q], near_recv.at[q, i // 2], near_to[i])

    def near_early(q):
        near_copy(q, 2).start()

        @pl.when(jnp.logical_not(up_wraps))
        def _():
            near_copy(q, 0).start()

        @pl.when(jnp.logical_not(down_wraps))
        def _():
            near_copy(q, 1).start()

    def near_late(q):
        @pl.when(up_wraps)
        def _():
            near_copy(q, 0).start()

        @pl.when(down_wraps)
        def _():
            near_copy(q, 1).start()

    def near_relay(q):
        near_wait(q, 0)
        near_copy(q, 3).start()

    def near_wait(q, part):
        two = near_x[q].at[pl.ds(0, 2)]
        remote(two, two, near_send.at[q], near_recv.at[q, part], twin).wait_recv()

    def make_plan():
        small[0].wait()

        def number(shape, dim):
            return lax.broadcasted_iota(jnp.int32, shape, dim)

        def total(mask, value, axis):
            return jnp.sum(jnp.where(mask, value, 0), axis=axis, keepdims=True, dtype=jnp.int32)

        square, wide, low = (SLOTS, SLOTS), (SLOTS, 128), (N_COL, 128)
        rows_on_lanes = jnp.broadcast_to(row_buf[...], square)
        i, j = number(square, 0), number(square, 1)
        rows = total(i == j, rows_on_lanes, 1)
        place = total((rows_on_lanes == rows) & (j < i), 1, 1)
        a = number(wide, 1)
        count = total(a == rows, 1, 0)
        groups = lax.shift_right_logical(count + (PACK - 1), 2)
        dest = PACK * total(a < rows, jnp.broadcast_to(groups, wide), 1) + place
        slot = number(wide, 0)
        uslot = total(dest == a, slot, 0)
        cslot = SLOTS + total(dest == a, slot - SLOTS, 0)
        b, lane = number(low, 0), number(low, 1)
        groups_low = jnp.broadcast_to(groups, low)
        own = total(b == lane, groups_low, 1)
        end = total(lane <= b, groups_low, 1)
        same = 1 - total((end - own == lane) & (own > 0), 1, 0)
        last = total(b == lane, jnp.where(own > 0, end, 0), 0)
        plan_buf[...] = jnp.concatenate([uslot, cslot, same, last] * 2, axis=0)
        copy = pltpu.make_async_copy(plan_buf, plan, plan_sem)
        copy.start()
        coef[SLOTS] = jnp.zeros((2 * RANK, PART), BF16)
        for n in range(2):
            part[n, 0] = jnp.zeros((TILE, PART), F32)
        copy.wait()

    def within(index, most):
        return jnp.minimum(jnp.maximum(index, 0), most)

    def group_u(w, g):
        stack = [u_buf[w, within(plan[0, PACK * g + i], SLOTS - 1)] for i in range(PACK)]
        ugrp[w, g] = jnp.concatenate(stack, axis=0).T

    def near_product(q):
        w = q // 2

        def rows(b, carry):
            here = pl.ds(pl.multiple_of(b * 128, 128), 128)
            real = jnp.zeros((128, PART), F32)
            imag = jnp.zeros((128, PART), F32)
            for n in range(NEAR):
                at = near_x[q][near_offset[0, n] + 2]
                real += jnp.dot(near_buf[w, n, 0, here], at, preferred_element_type=F32)
                imag += jnp.dot(near_buf[w, n, 1, here], at, preferred_element_type=F32)
            near_acc[q, here, :LANES] = real[:, :LANES] - imag[:, LANES:]
            near_acc[q, here, LANES:] = real[:, LANES:] + imag[:, :LANES]
            return carry

        lax.fori_loop(0, TILE // 128, rows, 0)

    rank_row = lax.broadcasted_iota(jnp.int32, (RANK, LANES), 0)

    def coefficients(q, s):
        at = tiles[q][far_col[0, s]]
        prod = jnp.dot(v_buf[q // 2, s], at, preferred_element_type=F32)
        live = rank_row < jnp.where(s < far_count[0, 0], far_rank[0, s], 0)
        real = jnp.where(live, prod[:RANK, :LANES] - prod[RANK:, LANES:], 0.0).astype(BF16)
        imag = jnp.where(live, prod[:RANK, LANES:] + prod[RANK:, :LANES], 0.0).astype(BF16)
        coef[s, :RANK, :LANES] = real
        coef[s, :RANK, LANES:] = imag
        coef[s, RANK:, :LANES] = -imag
        coef[s, RANK:, LANES:] = real

    def row_sums(q, g):
        sums = part.at[q % 2]
        same = plan[2, g].astype(F32)
        stack = [coef[within(plan[1, PACK * g + i], SLOTS)] for i in range(PACK)]
        right = jnp.concatenate(stack, axis=0)
        prod = jnp.dot(ugrp[q // 2, g], right, preferred_element_type=F32)
        sums[g + 1] = prod + same * sums[g]

    def row_part(q, a):
        return part[q % 2, within(plan[3, a], GROUPS)]

    def half_copy(q, i):
        return remote(half_out.at[q, i], half_in.at[q, i], half_send.at[q], half_recv.at[q, i], twin)

    upper, lower = pl.ds(0, 128), pl.ds(128, 128)
    moves = ((1, upper, far_up), (1, lower, far_down), (0, lower, far_up), (2, upper, far_down), (0, upper, far_up), (2, lower, far_down))

    def far_copy(q, m):
        d, rows, to = moves[m]
        return remote(far_out.at[q, d, rows], far_in.at[q, d, rows], far_send.at[q], far_recv.at[q, min(m // 2, 1)], to)

    turns = [mod(zh + step, 4) for step in (2, 1, 3, 0)]

    def reduce_pack(q):
        for n, i in enumerate(turns):
            half_out[q, i] = row_part(q, 2 * i + 1 - core).astype(BF16)
            if n:
                half_copy(q, turns[n - 1]).start()
        half_copy(q, turns[3]).start()

    def reduce_pass(q):
        for n, i in enumerate(turns):
            half_copy(q, i).wait_recv()
            both = row_part(q, 2 * i + core) + half_in[q, i].astype(F32)
            if n == 0:
                far_out[q, 1] = both.astype(BF16)
            elif n == 1:
                far_out[q, 0, lower] = both[128:].astype(BF16)
                held[q % 2, 0] = both[:128]
                far_copy(q, 0).start()
                far_copy(q, 1).start()
            elif n == 2:
                far_out[q, 2, upper] = both[:128].astype(BF16)
                held[q % 2, 1] = both[128:]
                far_copy(q, 2).start()
            else:
                own_acc[q] = both
                far_copy(q, 3).start()

    def reduce_relay(q):
        got = far_in.at[q, 1]
        remote(got, got, far_send.at[q], far_recv.at[q, 0], far_up).wait_recv()
        far_out[q, 0, upper] = (held[q % 2, 0] + far_in[q, 1, upper].astype(F32)).astype(BF16)
        far_out[q, 2, lower] = (held[q % 2, 1] + far_in[q, 1, lower].astype(F32)).astype(BF16)
        far_copy(q, 4).start()
        far_copy(q, 5).start()

    def finish(q):
        got = far_in.at[q, pl.ds(0, 2)]
        remote(got, got, far_send.at[q], far_recv.at[q, 1], far_up).wait_recv()
        total = near_acc[q] + own_acc[q] + far_in[q, 0].astype(F32) + far_in[q, 2].astype(F32)
        out_buf[q] = total.astype(BF16)
        for copy in out_copies(q):
            copy.start()

    def out_copies(q):
        return [
            pltpu.make_async_copy(
                out_buf.at[q, :, pl.ds(LANES * i, LANES)],
                out_hbm.at[q // 2, :, pl.ds(HALF * i + LANES * (q % 2), LANES)],
                out_sem.at[q],
            )
            for i in range(2)
        ]

    def many(first, last, step, *head, unroll=1):
        def one(i, carry):
            for n in range(unroll):
                step(*head, i * unroll + n)
            return carry

        lax.fori_loop(first // unroll, last // unroll, one, 0)

    def near_all(q):
        near_wait(q, 1)
        near_product(q)

    def pair_start(q):
        pair_copy(q, r).start()

    def near_own():
        for q in range(CHUNKS):
            pltpu.make_async_copy(near_x[q].at[2], near_x[q].at[2], x_sem.at[q, 1]).wait()

    def all_sent():
        for q in range(CHUNKS):
            ring_sent(q)
            pair_copy(q, r).wait_send()
            remote(half_out.at[q], half_in.at[q], half_send.at[q], half_recv.at[q, 0], twin).wait_send()
            four = near_x[q].at[pl.ds(0, 4)]
            remote(four, four, near_send.at[q], near_recv.at[q, 0], twin).wait_send()
            if q in SHORT:
                crossed = tiles[q].at[pl.ds(0, 1 + 2 * (HOPS - 1 - SHORT[q]))]
                remote(crossed, crossed, cross_send.at[q], cross_recv.at[q, 0], pair).wait_send()

    def load_chunk(q):
        pltpu.make_async_copy(tiles[q].at[r], tiles[q].at[r], x_sem.at[q, 0]).wait()

    load_chunk(0)
    pair_copy(0, r).start()
    forward(0, 0, 0)
    load_chunk(1)
    pair_copy(1, r).start()
    forward(1, 0, 0)
    load_chunk(2)
    load_chunk(3)
    def step(q, k, sub):
        if (q, k, sub) not in ((0, 0, 0), (1, 0, 0)):
            forward(q, k, sub)
        if (k, sub) == (6, 0):
            near_late(q)
        if (k, sub) == (7, 0) and SHORT.get(q) == 6:
            cross_start(q, 7)

    def group_piece(i):
        each = WAVES * GROUPS // G_PIECES
        many(each * i, each * i + each, lambda n: group_u(n // GROUPS, lax.rem(n, GROUPS)))

    def v_piece(q, i):
        each = SLOTS // V_PIECES
        many(each * i, each * i + each, coefficients, q, unroll=V_UNROLL)

    def u_piece(q, i):
        cuts = [GROUPS * n // U_PIECES for n in range(U_PIECES + 1)]
        many(cuts[i], cuts[i + 1], row_sums, q, unroll=U_UNROLL)

    def loaded():
        for load in small[1:] + [loads[0], loads[2]]:
            load.wait()
        near_own()

    run = {
        "step": step, "cross": cross, "drain": drain, "plan": make_plan, "u_loaded": loads[1].wait, "group": group_piece,
        "loaded": loaded, "near_early": near_early, "pair": pair_start, "V": v_piece, "U": u_piece, "pack": reduce_pack,
        "pass": reduce_pass, "relay": reduce_relay, "near_relay": near_relay, "near": near_all, "finish": finish,
    }
    for name in schedule():
        if name == ("finish", CHUNKS - 1):
            all_sent()
        with jax.named_scope("_".join(str(x) for x in name)):
            run[name[0]](*name[1:])
    for q in range(CHUNKS):
        remote(far_out.at[q], far_in.at[q], far_send.at[q], far_recv.at[q, 0], far_up).wait_send()
        pltpu.make_async_copy(out_buf.at[q], out_buf.at[q], out_sem.at[q]).wait()


def shards(incident, near_tiles, near_offsets, far_row, far_col, far_rank, far_count, far_u, far_v):
    dma = pltpu.SemaphoreType.DMA
    return pl.pallas_call(
        body,
        out_shape=jax.ShapeDtypeStruct((WAVES, TILE, WIDTH), BF16),
        in_specs=[pl.BlockSpec(memory_space=pl.ANY)] * 9,
        out_specs=pl.BlockSpec(memory_space=pl.ANY),
        scratch_shapes=[pltpu.VMEM((N_ROW, TILE, PART), BF16)] * CHUNKS
        + [pltpu.VMEM((5, TILE, PART), BF16)] * CHUNKS
        + [
            pltpu.VMEM((SLOTS + 1, 2 * RANK, PART), BF16),
            pltpu.VMEM((WAVES, GROUPS, TILE, PACK * 2 * RANK), BF16),
            pltpu.VMEM((WAVES, SLOTS, 2 * RANK, TILE), BF16),
            pltpu.VMEM((WAVES, SLOTS, 2 * RANK, TILE), BF16),
            pltpu.VMEM((WAVES, NEAR, 2, TILE, TILE), BF16),
            pltpu.VMEM((CHUNKS, TILE, PART), F32),
            pltpu.VMEM((2, GROUPS + 1, TILE, PART), F32),
            pltpu.VMEM((CHUNKS, 4, TILE, PART), BF16),
            pltpu.VMEM((CHUNKS, 4, TILE, PART), BF16),
            pltpu.VMEM((CHUNKS, 3, TILE, PART), BF16),
            pltpu.VMEM((CHUNKS, 3, TILE, PART), BF16),
            pltpu.VMEM((2, 2, 128, PART), F32),
            pltpu.VMEM((CHUNKS, TILE, PART), F32),
            pltpu.VMEM((CHUNKS, TILE, PART), BF16),
            pltpu.VMEM((1, SLOTS), jnp.int32),
            pltpu.VMEM((8, 128), jnp.int32),
            pltpu.SMEM((8, 128), jnp.int32),
            pltpu.SMEM((1, SLOTS), jnp.int32),
            pltpu.SMEM((1, SLOTS), jnp.int32),
            pltpu.SMEM((1, 1), jnp.int32),
            pltpu.SMEM((1, NEAR), jnp.int32),
            dma((5,)),
            dma,
            dma((CHUNKS, 2)),
            dma((3,)),
            dma((CHUNKS,)),
            dma((CHUNKS, HOPS, 2)),
            dma((CHUNKS,)),
            dma((CHUNKS,)),
            dma((CHUNKS,)),
            dma((CHUNKS, 2)),
            dma((CHUNKS,)),
            dma((CHUNKS, 4)),
            dma((CHUNKS,)),
            dma((CHUNKS, 2)),
            dma((CHUNKS,)),
            dma((CHUNKS, 2)),
            dma((CHUNKS,)),
        ],
        compiler_params=pltpu.CompilerParams(
            collective_id=0, has_side_effects=True, vmem_limit_bytes=67_043_328
        ),
    )(
        far_row[0],
        far_col[0],
        far_rank[0],
        far_count,
        near_offsets,
        incident,
        near_tiles[0],
        far_u[0, 0].reshape(WAVES, SLOTS, 2 * RANK, TILE),
        far_v[0, 0].reshape(WAVES, SLOTS, 2 * RANK, TILE),
    )


def solution(mesh):
    in_specs = (
        P(None, ("row", "col"), None),
        P(("row", "col"), None, None, None, None, None),
        P(("row", "col"), None),
        P("row", "col", None),
        P("row", "col", None),
        P("row", "col", None),
        P("row", "col"),
        P("row", "col", None, None, None, None, None),
        P("row", "col", None, None, None, None, None),
    )
    out_specs = P(None, ("row", "col"), None)
    return jax.shard_map(shards, mesh=mesh, in_specs=in_specs, out_specs=out_specs, check_vma=False)
```
